32 devices in a mesh: dp: 8 (over z, y), tensor: 4 (over x, core).
Axes of the slice: x: 2, y: 2, z: 4, core: 2. Of those that a mesh axis runs over, the one named last changes fastest.
Arguments:
- inputs: float32 [12288, 768], P(('dp', 'tensor')), may hold values from -40 to 40
- cotangent: float32 [12288, 768], P(('dp', 'tensor')), may hold values from -12 to 12
- clip_lengths: int32 [12], replicated, may hold values from 1 to 1500, 12288 in all
- inward_weight: float32 [768, 3, 768], P('dp', None, 'tensor'), may hold values from -0.5 to 0.5
- outward_weight: float32 [768, 768], P('tensor', 'dp'), may hold values from -0.875 to 0.875
- expand_weight: float32 [768, 3072], P('dp', 'tensor'), may hold values from -0.21875 to 0.21875
- shrink_weight: float32 [3072, 768], P('tensor', 'dp'), may hold values from -0.109375 to 0.109375
- gains: float32 [2, 768], P(None, ('dp', 'tensor')), may hold values from 0.5 to 1.5
- shifts: float32 [2, 768], P(None, ('dp', 'tensor')), may hold values from -1.75 to 1.75
- biases: float32 [4, 768], P(None, ('dp', 'tensor')), may hold values from -1.75 to 1.75
- expand_bias: float32 [3072], P(('dp', 'tensor')), may hold values from -1.75 to 1.75
- inward_moment: float32 [768, 3, 768], P('dp', None, 'tensor'), may hold values from -199.53225 to 199.53225
- outward_moment: float32 [768, 768], P('tensor', 'dp'), may hold values from -199.53225 to 199.53225
- expand_moment: float32 [768, 3072], P('dp', 'tensor'), may hold values from -199.53225 to 199.53225
- shrink_moment: float32 [3072, 768], P('tensor', 'dp'), may hold values from -199.53225 to 199.53225
- gains_moment: float32 [2, 768], P(None, ('dp', 'tensor')), may hold values from -128 to 128
- shifts_moment: float32 [2, 768], P(None, ('dp', 'tensor')), may hold values from -128 to 128
- biases_moment: float32 [4, 768], P(None, ('dp', 'tensor')), may hold values from -128 to 128
- expand_bias_moment: float32 [3072], P(('dp', 'tensor')), may hold values from -128 to 128
Outputs:
- output: float32 [12288, 768], P(('dp', 'tensor'))
- input_grad: float32 [12288, 768], P(('dp', 'tensor'))
- inward_grad: float32 [768, 3, 768], P('dp', None, 'tensor')
- outward_grad: float32 [768, 768], P('tensor', 'dp')
- expand_grad: float32 [768, 3072], P('dp', 'tensor')
- shrink_grad: float32 [3072, 768], P('tensor', 'dp')
- gains_grad: float32 [2, 768], P(None, ('dp', 'tensor'))
- shifts_grad: float32 [2, 768], P(None, ('dp', 'tensor'))
- biases_grad: float32 [4, 768], P(None, ('dp', 'tensor'))
- expand_bias_grad: float32 [3072], P(('dp', 'tensor'))
- inward_new: float32 [768, 3, 768], P('dp', None, 'tensor')
- outward_new: float32 [768, 768], P('tensor', 'dp')
- expand_new: float32 [768, 3072], P('dp', 'tensor')
- shrink_new: float32 [3072, 768], P('tensor', 'dp')
- gains_new: float32 [2, 768], P(None, ('dp', 'tensor'))
- shifts_new: float32 [2, 768], P(None, ('dp', 'tensor'))
- biases_new: float32 [4, 768], P(None, ('dp', 'tensor'))
- expand_bias_new: float32 [3072], P(('dp', 'tensor'))
- inward_state: float32 [768, 3, 768], P('dp', None, 'tensor')
- outward_state: float32 [768, 768], P('tensor', 'dp')
- expand_state: float32 [768, 3072], P('dp', 'tensor')
- shrink_state: float32 [3072, 768], P('tensor', 'dp')
- gains_state: float32 [2, 768], P(None, ('dp', 'tensor'))
- shifts_state: float32 [2, 768], P(None, ('dp', 'tensor'))
- biases_state: float32 [4, 768], P(None, ('dp', 'tensor'))
- expand_bias_state: float32 [3072], P(('dp', 'tensor'))
The draws below stay inside these ranges and needn't reach their ends.
Inputs may be any that keep to these rules, and one draw needn't show every extreme that they name: `clip_lengths`: clips lie end to end in token order and together fill all 12288 tokens; the longest has exactly 1500 frames.
All inputs are finite; a program needn't handle non-finite values.
Results may differ from the reference program's by a relative error of at most 0.033.
Values may be sent and summed in bfloat16 or wider, within the bound.
A program may use at most 256 MiB of HBM per device.

```python
import math
import jax
import jax.numpy as jnp
import numpy as np
from jax import lax

D = 768
HEADS = 12
HDIM = 64
FF = 3072
MAXCLIP = 1500
NS_STEPS = 3
RUN = 1536
TOKENS = 12288
CLIPS = 12


def log_spread(key, count, low, high):
    return jnp.exp(jax.random.uniform(key, (count,), jnp.float32, jnp.log(low), jnp.log(high)))


def draw_inputs(key, part):
    keys = jax.random.split(jax.random.fold_in(key, 11), 3)
    noise = jnp.clip(jax.random.normal(keys[0], (TOKENS, D), jnp.float32), -4.0, 4.0)
    scales = log_spread(keys[1], TOKENS, 0.3, 3.0)
    columns = log_spread(keys[2], D, 0.3, 3.0)
    return noise * scales[:, None] * columns[None, :]


def draw_cotangent(key, part):
    keys = jax.random.split(jax.random.fold_in(key, 17), 2)
    rising = 0.5 + jnp.arange(TOKENS, dtype=jnp.float32) / TOKENS
    noise = jnp.clip(jax.random.normal(keys[0], (TOKENS, D), jnp.float32), -4.0, 4.0)
    scales = log_spread(keys[1], TOKENS, 0.5, 2.0)
    return noise * (rising * scales)[:, None]


def draw_inward_weight(key, part):
    keys = jax.random.split(jax.random.fold_in(key, 13), 1)
    return jnp.clip(jax.random.normal(keys[0], (D, 3, D), jnp.float32), -4.0, 4.0) / D ** 0.5


def spread_matrix(key, height, width):
    keys = jax.random.split(key, 3)
    level = 0.05 * TOKENS ** 0.5
    noise = jnp.clip(jax.random.normal(keys[0], (height, width), jnp.float32), -4.0, 4.0)
    scales = log_spread(keys[1], height, 0.3, 3.0)
    columns = log_spread(keys[2], width, 0.3, 3.0)
    return level * noise * scales[:, None] * columns[None, :]


def draw_inward_moment(key, part):
    return spread_matrix(jax.random.fold_in(key, 21), D, 3 * D).reshape(D, 3, D)


def draw_outward_moment(key, part):
    return spread_matrix(jax.random.fold_in(key, 22), D, D)


def draw_expand_moment(key, part):
    return spread_matrix(jax.random.fold_in(key, 23), D, FF)


def draw_shrink_moment(key, part):
    return spread_matrix(jax.random.fold_in(key, 24), FF, D)


def level_of(key, dims, cuts, smallest, high):
    level, own = 1.0, jax.random.fold_in(key, 6)
    for dim, blocks in cuts:
        steps = jnp.exp(jax.random.uniform(jax.random.fold_in(own, dim), (blocks,), jnp.float32, smallest / len(cuts), high / len(cuts)))
        level = level * jnp.repeat(steps, dims[dim] // blocks).reshape([-1 if axis == dim else 1 for axis in range(len(dims))])
    return level


def profile(count, total, bound, skew):
    portions = [(1 << 20) // math.isqrt(standing ** skew) + 1 for standing in range(2, count + 1)]
    surplus, holding = total - bound - (count - 1), [1] * (count - 1)
    while surplus > 0:
        free = [i for i in range(count - 1) if holding[i] < bound]
        mass, budget = sum([portions[i] for i in free]), surplus
        for i in free:
            extra = min(bound - holding[i], max(1, budget * portions[i] // mass), surplus)
            holding[i] = holding[i] + extra
            surplus = surplus - extra
    return np.array([bound] + holding)


def ragged(stream_key, count, total, bound, skew):
    if count == 2:
        one = jax.random.randint(stream_key, (), max(1, total - bound), min(bound, total - 1) + 1)
        return jnp.stack([one, total - one])
    lengths = jnp.asarray(profile(count, total, bound, skew), jnp.int32)
    pairs = (count - 1) // 2
    donor, receiver = lengths[1:1 + 2 * pairs:2], lengths[2:2 + 2 * pairs:2]
    margin = jnp.minimum(donor - 1, bound - receiver)
    shifted = jax.random.randint(jax.random.fold_in(stream_key, 1), (pairs,), 0, 1 << 20) % (margin + 1)
    lengths = lengths.at[1:1 + 2 * pairs:2].set(donor - shifted).at[2:2 + 2 * pairs:2].set(receiver + shifted)
    return lengths[jax.random.permutation(jax.random.fold_in(stream_key, 2), count)]


def centred(rng, extent, scale, reach, shards=(), kind=jnp.bfloat16):
    factor_of = level_of(rng, extent, shards, -0.22, 0.18) if shards else 1.0
    values = jax.random.normal(rng, extent, jnp.float32) * scale * factor_of
    return jnp.minimum(jnp.maximum(values, -reach), reach).astype(kind)


def setup_inputs(seed: int = 0) -> dict:
    splits = jax.random.split(jax.random.key(seed), 20)
    return {
        "inputs": draw_inputs(jax.random.fold_in(splits[19], 71), 0),
        "cotangent": draw_cotangent(jax.random.fold_in(splits[19], 71), 0),
        "clip_lengths": ragged(splits[2], CLIPS, TOKENS, MAXCLIP, 1).astype(jnp.int32),
        "inward_weight": draw_inward_weight(jax.random.fold_in(splits[19], 71), 0),
        "outward_weight": centred(splits[4], (D, D), (D // 16) ** -0.5, 0.875, ((0, 4), (1, 8)), jnp.float32),
        "expand_weight": centred(splits[5], (D, FF), D ** -0.5, 0.21875, ((0, 8), (1, 4)), jnp.float32),
        "shrink_weight": centred(splits[6], (FF, D), FF ** -0.5, 0.109375, ((0, 4), (1, 8)), jnp.float32),
        "gains": jnp.clip(1.0 + 0.1 * jax.random.normal(splits[7], (2, D), jnp.float32), 0.5, 1.5),
        "shifts": centred(splits[8], (2, D), 0.3, 1.75, ((1, 32),), jnp.float32),
        "biases": centred(splits[9], (4, D), 0.3, 1.75, ((1, 32),), jnp.float32),
        "expand_bias": centred(splits[10], (FF,), 0.3, 1.75, ((0, 32),), jnp.float32),
        "inward_moment": draw_inward_moment(jax.random.fold_in(splits[19], 71), 0),
        "outward_moment": draw_outward_moment(jax.random.fold_in(splits[19], 71), 0),
        "expand_moment": draw_expand_moment(jax.random.fold_in(splits[19], 71), 0),
        "shrink_moment": draw_shrink_moment(jax.random.fold_in(splits[19], 71), 0),
        "gains_moment": centred(splits[15], (2, D), (0.2 * TOKENS ** 0.5), 128.0, ((1, 32),), jnp.float32),
        "shifts_moment": centred(splits[16], (2, D), (0.2 * TOKENS ** 0.5), 128.0, ((1, 32),), jnp.float32),
        "biases_moment": centred(splits[17], (4, D), (0.2 * TOKENS ** 0.5), 128.0, ((1, 32),), jnp.float32),
        "expand_bias_moment": centred(splits[18], (FF,), (0.2 * TOKENS ** 0.5), 128.0, ((0, 32),), jnp.float32),
    }


norm_epsilon = 1e-05
frobenius_epsilon = 1e-07
quintic_one = 3.4445
quintic_two = -4.775
quintic_three = 2.0315
momentum_decay = 0.9
learn_rate = 0.2
vector_rate = 0.003
masked_score = -1e+30
root_half = 0.7071067811865476
gauss_factor = 0.3989422804014327

def normalize(values_in):
    center = values_in - lax.optimization_barrier(jnp.mean(values_in, axis=-1, keepdims=True))
    inverse = lax.rsqrt(lax.optimization_barrier(jnp.mean(center * center, axis=-1, keepdims=True)) + norm_epsilon)
    return (center * inverse, inverse)

def norm_back(grad_rows, unit, inverse, gain):
    scaled = grad_rows * gain
    return inverse * (scaled - lax.optimization_barrier(jnp.mean(scaled, axis=-1, keepdims=True)) - unit * lax.optimization_barrier(jnp.mean(scaled * unit, axis=-1, keepdims=True)))

def gelu_value(pre):
    return pre * 0.5 * (1.0 + lax.erf(pre * root_half))

def gelu_slope(pre):
    return 0.5 * (1.0 + lax.erf(pre * root_half)) + pre * jnp.exp(-0.5 * pre * pre) * gauss_factor

def clip_index(clip_lengths, positions, total):
    ends = jnp.cumsum(clip_lengths, dtype=jnp.int32)
    found = lax.optimization_barrier(jnp.sum((ends[None, :] <= positions[:, None]).astype(jnp.int32), axis=1, dtype=jnp.int32))
    inside = (positions >= 0) & (positions < total)
    return jnp.where(inside, found, -1).astype(jnp.int32)

def orthogonalize(matrix):
    rounded = matrix.astype(jnp.bfloat16)
    wide = lax.optimization_barrier(rounded).astype(jnp.float32)
    state = (wide / (jnp.sqrt(jnp.sum(wide * wide)) + frobenius_epsilon)).astype(jnp.bfloat16)
    for sweep in range(NS_STEPS):
        gram = jnp.dot(state, state.T, preferred_element_type=jnp.float32).astype(jnp.bfloat16)
        poly = (quintic_two * lax.optimization_barrier(gram).astype(jnp.float32) + quintic_three * jnp.dot(gram, gram, preferred_element_type=jnp.float32)).astype(jnp.bfloat16)
        state = (quintic_one * lax.optimization_barrier(state).astype(jnp.float32) + jnp.dot(poly, state, preferred_element_type=jnp.float32)).astype(jnp.bfloat16)
    return state

def block_parts(query, key_pad, value_pad, query_tags, key_tags, index, block_rows, window):
    start = index * block_rows
    query_rows = lax.dynamic_slice_in_dim(query, start, block_rows, 0).astype(jnp.float32).reshape(block_rows, HEADS, HDIM)
    key_rows = lax.dynamic_slice_in_dim(key_pad, start, window, 0).astype(jnp.float32).reshape(window, HEADS, HDIM)
    value_rows = lax.dynamic_slice_in_dim(value_pad, start, window, 0).astype(jnp.float32).reshape(window, HEADS, HDIM)
    allowed = lax.dynamic_slice_in_dim(query_tags, start, block_rows)[:, None] == lax.dynamic_slice_in_dim(key_tags, start, window)[None, :]
    score = jnp.where(allowed[None], jnp.einsum('qhd,khd->hqk', query_rows, key_rows) / math.sqrt(HDIM), masked_score)
    return (start, query_rows, key_rows, value_rows, score)

def attend_forward(query, key_pad, value_pad, query_tags, key_tags):
    block_rows = min(512, RUN)
    window = block_rows + 2 * MAXCLIP

    def one_block(index):
        start, query_rows, key_rows, value_rows, score = block_parts(query, key_pad, value_pad, query_tags, key_tags, index, block_rows, window)
        top = lax.optimization_barrier(jnp.max(score, axis=2, keepdims=True))
        log_total = top + jnp.log(lax.optimization_barrier(jnp.sum(jnp.exp(score - top), axis=2, keepdims=True)))
        probs = jnp.exp(score - log_total).astype(jnp.bfloat16)
        mixed = jnp.einsum('hqk,khd->qhd', lax.optimization_barrier(probs).astype(jnp.float32), value_rows)
        return (mixed.reshape(block_rows, D).astype(jnp.bfloat16), log_total[:, :, 0])
    blocks, totals = lax.map(one_block, jnp.arange(TOKENS // block_rows, dtype=jnp.int32))
    return (blocks.reshape(TOKENS, D), totals)

def attend_backward(query, key_pad, value_pad, query_tags, key_tags, attended, totals, attended_grad):
    block_rows = min(512, RUN)
    window = block_rows + 2 * MAXCLIP
    scale = 1.0 / math.sqrt(HDIM)

    def one_block(carry, inputs_now):
        index, log_total = inputs_now
        start, query_rows, key_rows, value_rows, score = block_parts(query, key_pad, value_pad, query_tags, key_tags, index, block_rows, window)
        exact = jnp.exp(score - log_total[:, :, None])
        probs = exact.astype(jnp.bfloat16)
        grad_out = lax.dynamic_slice_in_dim(attended_grad, start, block_rows, 0).astype(jnp.float32).reshape(block_rows, HEADS, HDIM)
        out_rows = lax.dynamic_slice_in_dim(attended, start, block_rows, 0).astype(jnp.float32).reshape(block_rows, HEADS, HDIM)
        delta = lax.optimization_barrier(jnp.sum(grad_out * out_rows, axis=2))
        prob_grad = jnp.einsum('qhd,khd->hqk', grad_out, value_rows)
        score_grad = (exact * (prob_grad - delta.T[:, :, None])).astype(jnp.bfloat16)
        score_wide = lax.optimization_barrier(score_grad).astype(jnp.float32)
        query_grad = jnp.einsum('hqk,khd->qhd', score_wide, key_rows) * scale
        key_grad = jnp.einsum('hqk,qhd->khd', score_wide, query_rows) * scale
        value_grad = jnp.einsum('hqk,qhd->khd', lax.optimization_barrier(probs).astype(jnp.float32), grad_out)
        update = jnp.concatenate([key_grad.reshape(window, D), value_grad.reshape(window, D)], axis=1)
        current = lax.dynamic_slice_in_dim(carry, start, window, 0)
        carry = lax.dynamic_update_slice_in_dim(carry, current + update, start, 0)
        return (carry, query_grad.reshape(block_rows, D))
    initial = jnp.zeros((TOKENS + 2 * MAXCLIP, 2 * D), jnp.float32)
    pair_grads, query_blocks = lax.scan(one_block, initial, (jnp.arange(TOKENS // block_rows, dtype=jnp.int32), totals))
    inner = pair_grads[MAXCLIP:MAXCLIP + TOKENS]
    return (query_blocks.reshape(TOKENS, D), inner[:, :D], inner[:, D:])

def matrix_step(weight, moment, grad, turned):
    state = momentum_decay * moment + grad
    flat = state.reshape(state.shape[0], -1)
    if turned:
        ortho = orthogonalize(flat.T).T
    else:
        ortho = orthogonalize(flat)
    factor = learn_rate * 0.2 * math.sqrt(max(flat.shape[0], flat.shape[1]))
    return (weight - factor * ortho.astype(jnp.float32).reshape(weight.shape), state)

def reference(inputs, cotangent, clip_lengths, inward_weight, outward_weight, expand_weight, shrink_weight, gains, shifts, biases, expand_bias, inward_moment, outward_moment, expand_moment, shrink_moment, gains_moment, shifts_moment, biases_moment, expand_bias_moment):
    query_tags = clip_index(clip_lengths, jnp.arange(TOKENS, dtype=jnp.int32), TOKENS)
    key_tags = clip_index(clip_lengths, jnp.arange(TOKENS + 2 * MAXCLIP, dtype=jnp.int32) - MAXCLIP, TOKENS)
    inward_b = inward_weight.astype(jnp.bfloat16).reshape(D, 3 * D)
    outward_b = outward_weight.astype(jnp.bfloat16)
    expand_b = expand_weight.astype(jnp.bfloat16)
    shrink_b = shrink_weight.astype(jnp.bfloat16)
    unit_one, inverse_one = normalize(inputs)
    normed_one = (unit_one * gains[0] + shifts[0]).astype(jnp.bfloat16)
    mixed = jnp.dot(normed_one, inward_b, preferred_element_type=jnp.float32).reshape(TOKENS, 3, D)
    query = (mixed[:, 0] + biases[0]).astype(jnp.bfloat16)
    keys = mixed[:, 1].astype(jnp.bfloat16)
    values = (mixed[:, 2] + biases[1]).astype(jnp.bfloat16)
    key_pad = jnp.pad(keys, ((MAXCLIP, MAXCLIP), (0, 0)))
    value_pad = jnp.pad(values, ((MAXCLIP, MAXCLIP), (0, 0)))
    attended, totals = attend_forward(query, key_pad, value_pad, query_tags, key_tags)
    mid = inputs + jnp.dot(attended, outward_b, preferred_element_type=jnp.float32) + biases[2]

    def feed_block(carry, block):
        mid_rows, grad_rows = block
        unit_two, inverse_two = normalize(mid_rows)
        normed_two = (unit_two * gains[1] + shifts[1]).astype(jnp.bfloat16)
        pre = jnp.dot(normed_two, expand_b, preferred_element_type=jnp.float32) + expand_bias
        act = gelu_value(pre).astype(jnp.bfloat16)
        out_rows = mid_rows + jnp.dot(act, shrink_b, preferred_element_type=jnp.float32) + biases[3]
        grad_b = grad_rows.astype(jnp.bfloat16)
        pre_grad = jnp.dot(grad_b, shrink_b.T, preferred_element_type=jnp.float32) * gelu_slope(pre)
        pre_grad_b = pre_grad.astype(jnp.bfloat16)
        normed_two_grad = jnp.dot(pre_grad_b, expand_b.T, preferred_element_type=jnp.float32)
        mid_grad_rows = grad_rows + norm_back(normed_two_grad, unit_two, inverse_two, gains[1])
        shrink_sum, expand_sum, hidden_sum, gain_sum, shift_sum = carry
        carry = (shrink_sum + jnp.dot(act.T, grad_b, preferred_element_type=jnp.float32), expand_sum + jnp.dot(normed_two.T, pre_grad_b, preferred_element_type=jnp.float32), hidden_sum + lax.optimization_barrier(jnp.sum(pre_grad, axis=0)), gain_sum + lax.optimization_barrier(jnp.sum(normed_two_grad * unit_two, axis=0)), shift_sum + lax.optimization_barrier(jnp.sum(normed_two_grad, axis=0)))
        return (carry, (out_rows, mid_grad_rows))
    initial = (jnp.zeros((FF, D), jnp.float32), jnp.zeros((D, FF), jnp.float32), jnp.zeros((FF,), jnp.float32), jnp.zeros((D,), jnp.float32), jnp.zeros((D,), jnp.float32))
    sums, (out_blocks, mid_blocks) = lax.scan(feed_block, initial, (mid.reshape(TOKENS // RUN, RUN, D), cotangent.reshape(TOKENS // RUN, RUN, D)))
    shrink_grad, expand_grad, expand_bias_grad, gain_two, shift_two = sums
    output = out_blocks.reshape(TOKENS, D)
    mid_grad = mid_blocks.reshape(TOKENS, D)
    mid_grad_b = mid_grad.astype(jnp.bfloat16)
    outward_grad = jnp.dot(attended.T, mid_grad_b, preferred_element_type=jnp.float32)
    attended_grad = jnp.dot(mid_grad_b, outward_b.T, preferred_element_type=jnp.float32).astype(jnp.bfloat16)
    query_grad, key_grad, value_grad = attend_backward(query, key_pad, value_pad, query_tags, key_tags, attended, totals, attended_grad)
    mixed_grad = jnp.stack([query_grad, key_grad, value_grad], axis=1).astype(jnp.bfloat16).reshape(TOKENS, 3 * D)
    inward_grad = jnp.dot(normed_one.T, mixed_grad, preferred_element_type=jnp.float32).reshape(D, 3, D)
    normed_one_grad = jnp.dot(mixed_grad, inward_b.T, preferred_element_type=jnp.float32)
    input_grad = mid_grad + norm_back(normed_one_grad, unit_one, inverse_one, gains[0])
    gains_grad = jnp.stack([lax.optimization_barrier(jnp.sum(normed_one_grad * unit_one, axis=0)), gain_two])
    shifts_grad = jnp.stack([lax.optimization_barrier(jnp.sum(normed_one_grad, axis=0)), shift_two])
    biases_grad = jnp.stack([lax.optimization_barrier(jnp.sum(query_grad, axis=0)), lax.optimization_barrier(jnp.sum(value_grad, axis=0)), lax.optimization_barrier(jnp.sum(mid_grad, axis=0)), lax.optimization_barrier(jnp.sum(cotangent, axis=0))])
    inward_new, inward_state = matrix_step(inward_weight, inward_moment, inward_grad, False)
    outward_new, outward_state = matrix_step(outward_weight, outward_moment, outward_grad, False)
    expand_new, expand_state = matrix_step(expand_weight, expand_moment, expand_grad, False)
    shrink_new, shrink_state = matrix_step(shrink_weight, shrink_moment, shrink_grad, True)
    gains_state = momentum_decay * gains_moment + gains_grad
    shifts_state = momentum_decay * shifts_moment + shifts_grad
    biases_state = momentum_decay * biases_moment + biases_grad
    expand_bias_state = momentum_decay * expand_bias_moment + expand_bias_grad
    gains_new = gains - vector_rate * gains_state
    shifts_new = shifts - vector_rate * shifts_state
    biases_new = biases - vector_rate * biases_state
    expand_bias_new = expand_bias - vector_rate * expand_bias_state
    return (output, input_grad, inward_grad, outward_grad, expand_grad, shrink_grad, gains_grad, shifts_grad, biases_grad, expand_bias_grad, inward_new, outward_new, expand_new, shrink_new, gains_new, shifts_new, biases_new, expand_bias_new, inward_state, outward_state, expand_state, shrink_state, gains_state, shifts_state, biases_state, expand_bias_state)
```

```python
import functools
import math

import jax
import jax.numpy as jnp
from jax import lax
from jax.experimental import pallas as pl
from jax.experimental.pallas import tpu as pltpu
from jax.sharding import PartitionSpec as P

HDIM = 64
MAXCLIP = 1500
NS_STEPS = 3
LANES = 128
NEG = -1e30

norm_epsilon = 1e-05
frobenius_epsilon = 1e-07
quintic_one = 3.4445
quintic_two = -4.775
quintic_three = 2.0315
momentum_decay = 0.9
learn_rate = 0.2
vector_rate = 0.003
root_half = 0.7071067811865476
gauss_factor = 0.3989422804014327


def over_last(left, right):
    return lax.dot_general(left, right, (((1,), (1,)), ((), ())), preferred_element_type=jnp.float32)


def over_first(left, right):
    return lax.dot_general(left, right, (((0,), (0,)), ((), ())), preferred_element_type=jnp.float32)


def picker(shape, heads, head, inner, flip):
    packed = lax.broadcasted_iota(jnp.int32, shape, 0 if not flip else 1)
    slot = lax.broadcasted_iota(jnp.int32, shape, 1 if not flip else 0)
    hit = (packed - head * HDIM == slot - inner) & (slot >= inner) & (slot < inner + HDIM)
    return jnp.where(hit, 1.0, 0.0).astype(jnp.bfloat16)


def clip_rows(clips_ref, count, cols, first):
    pos = first + lax.broadcasted_iota(jnp.int32, (1, cols), 1)

    def step(i, carry):
        end, start_row, end_row = carry
        stop = end + clips_ref[i]
        inside = (pos >= end) & (pos < stop)
        return stop, jnp.where(inside, end, start_row), jnp.where(inside, stop, end_row)

    zero = jnp.zeros((1, cols), jnp.int32)
    return lax.fori_loop(0, count, step, (jnp.int32(0), zero, zero))[1:]


def clip_span(clips_ref, count, first, last):
    def step(i, carry):
        end, low, high = carry
        stop = end + clips_ref[i]
        low = jnp.where((first >= end) & (first < stop), end, low)
        high = jnp.where((last >= end) & (last < stop), stop, high)
        return stop, low, high

    return lax.fori_loop(0, count, step, (jnp.int32(0), jnp.int32(0), jnp.int32(0)))[1:]


def block_bias(start_row, end_row, key_first, bk, bq):
    key = key_first + lax.broadcasted_iota(jnp.int32, (bk, bq), 0)
    return jnp.where((key >= start_row) & (key < end_row), 0.0, NEG)


def forward_body(heads, bq, bk, count, clips_ref, base_ref, q_ref, kv_ref, o_ref, lse_ref):
    run = q_ref.shape[0]
    base = base_ref[0]
    ext = base - run

    @pl.loop(0, run // bq)
    def _(i):
        first = base + i * bq
        rows = pl.ds(pl.multiple_of(i * bq, bq), bq)
        start_row, end_row = clip_rows(clips_ref, count, bq, first)
        low, high = clip_span(clips_ref, count, first, first + bq - 1)
        lo = (low - ext) // bk
        hi = (high - ext + bk - 1) // bk

        def step(j, carry):
            bias = block_bias(start_row, end_row, ext + j * bk, bk, bq)
            keys = pl.ds(pl.multiple_of(j * bk, bk), bk)
            out = []
            for head in range(heads):
                m, l, acc = carry[head]
                cols = slice(head * LANES, (head + 1) * LANES)
                kv = kv_ref[keys, cols]
                s = over_last(kv, q_ref[rows, cols]) + bias
                m_new = jnp.maximum(m, jnp.max(s, axis=0, keepdims=True))
                p = jnp.exp(s - m_new)
                alpha = jnp.exp(m - m_new)
                l = l * alpha + jnp.sum(p, axis=0, keepdims=True)
                acc = acc * alpha + over_first(kv, p.astype(jnp.bfloat16))
                out.append((m_new, l, acc))
            return tuple(out)

        init = tuple(
            (jnp.full((1, bq), NEG, jnp.float32), jnp.zeros((1, bq), jnp.float32), jnp.zeros((LANES, bq), jnp.float32))
            for _ in range(heads)
        )
        final = lax.fori_loop(lo, hi, step, init)
        total = None
        lse = []
        for head in range(heads):
            m, l, acc = final[head]
            o = (acc / l).astype(jnp.bfloat16)
            part = over_first(o, picker((LANES, heads * HDIM), heads, head, HDIM, True))
            total = part if total is None else total + part
            lse.append(m + jnp.log(l))
        lse.append(jnp.zeros((8 - heads, bq), jnp.float32))
        o_ref[rows, :] = total.astype(jnp.bfloat16)
        lse_ref[:, rows] = jnp.concatenate(lse, axis=0)


def backward_body(heads, bq, bk, count, clips_ref, base_ref, q_ref, kv_ref, o_ref, do_ref, lse_ref,
                  dq_ref, own_ref, rim_ref, sums_ref, dkv_ref, doz_ref):
    run = q_ref.shape[0]
    base = base_ref[0]
    ext = base - run
    scale = 1.0 / math.sqrt(HDIM)
    width = heads * HDIM
    dkv_ref[...] = jnp.zeros_like(dkv_ref)

    @pl.loop(0, run // bq)
    def _(i):
        first = base + i * bq
        rows = pl.ds(pl.multiple_of(i * bq, bq), bq)
        start_row, end_row = clip_rows(clips_ref, count, bq, first)
        low, high = clip_span(clips_ref, count, first, first + bq - 1)
        lo = (low - ext) // bk
        hi = (high - ext + bk - 1) // bk
        do = do_ref[rows, :]
        prod = do.astype(jnp.float32) * o_ref[rows, :].astype(jnp.float32)
        prod_hi = prod.astype(jnp.bfloat16)
        prod_lo = (prod - prod_hi.astype(jnp.float32)).astype(jnp.bfloat16)
        sel_row = lax.broadcasted_iota(jnp.int32, (8, width), 0)
        sel_col = lax.broadcasted_iota(jnp.int32, (8, width), 1)
        sel = jnp.where((sel_col >= sel_row * HDIM) & (sel_col < (sel_row + 1) * HDIM), 1.0, 0.0).astype(jnp.bfloat16)
        delta = over_last(sel, prod_hi) + over_last(sel, prod_lo)
        lse = lse_ref[:, rows]
        for head in range(heads):
            doz_ref[:, head * LANES:(head + 1) * LANES] = jnp.dot(
                do, picker((width, LANES), heads, head, HDIM, False), preferred_element_type=jnp.float32
            ).astype(jnp.bfloat16)

        def step(j, carry):
            bias = block_bias(start_row, end_row, ext + j * bk, bk, bq)
            keys = pl.ds(pl.multiple_of(j * bk, bk), bk)
            out = []
            for head in range(heads):
                cols = slice(head * LANES, (head + 1) * LANES)
                kv = kv_ref[keys, cols]
                qs = q_ref[rows, cols]
                doz = doz_ref[:, cols]
                p = jnp.exp(over_last(kv, qs) + bias - lse[head:head + 1])
                ds = (p * (over_last(kv, doz) - delta[head:head + 1])).astype(jnp.bfloat16)
                dkv_ref[keys, cols] += jnp.dot(ds, qs, preferred_element_type=jnp.float32) + jnp.dot(
                    p.astype(jnp.bfloat16), doz, preferred_element_type=jnp.float32)
                out.append(carry[head] + over_first(kv, ds))
            return tuple(out)

        init = tuple(jnp.zeros((LANES, bq), jnp.float32) for _ in range(heads))
        final = lax.fori_loop(lo, hi, step, init)
        for head in range(heads):
            dq_ref[rows, head * LANES:(head + 1) * LANES] = (final[head] * scale).T.astype(jnp.bfloat16)
    own_ref[...] = dkv_ref[pl.ds(run, run), :]
    rim_ref[0] = dkv_ref[pl.ds(0, run), :].astype(jnp.bfloat16)
    rim_ref[1] = dkv_ref[pl.ds(2 * run, run), :].astype(jnp.bfloat16)
    sums_ref[...] = jnp.zeros_like(sums_ref)


VM = pl.BlockSpec(memory_space=pltpu.VMEM)
SM = pl.BlockSpec(memory_space=pltpu.SMEM)


def attend_forward(clips, base, q, kv, heads, bq, bk):
    run = q.shape[0]
    return pl.pallas_call(
        functools.partial(forward_body, heads, bq, bk, clips.shape[0]),
        out_shape=(jax.ShapeDtypeStruct((run, heads * HDIM), jnp.bfloat16), jax.ShapeDtypeStruct((8, run), jnp.float32)),
        in_specs=[SM, SM, VM, VM],
        out_specs=(VM, VM),
        name="attend_forward",
    )(clips, base, q, kv)


def attend_backward(clips, base, q, kv, o, do, lse, heads, bq, bk):
    run = q.shape[0]
    wide = heads * LANES
    return pl.pallas_call(
        functools.partial(backward_body, heads, bq, bk, clips.shape[0]),
        out_shape=(
            jax.ShapeDtypeStruct((run, wide), jnp.bfloat16),
            jax.ShapeDtypeStruct((run, wide), jnp.float32),
            jax.ShapeDtypeStruct((2, run, wide), jnp.bfloat16),
            jax.ShapeDtypeStruct((8, wide), jnp.float32),
        ),
        in_specs=[SM, SM, VM, VM, VM, VM, VM],
        out_specs=(VM, VM, VM, VM),
        scratch_shapes=[pltpu.VMEM((3 * run, wide), jnp.float32), pltpu.VMEM((bq, wide), jnp.bfloat16)],
        name="attend_backward",
    )(clips, base, q, kv, o, do, lse)


class Seat:
    def __init__(self, data_count):
        self.planes = data_count // 2
        self.d = lax.axis_index("dp")
        self.t = lax.axis_index("tensor")
        self.h, self.l = self.d // 2, self.d % 2
        self.x, self.c = self.t // 2, self.t % 2
        self.run = 2 * self.h + self.c
        self.spot = 4 * self.l + self.t


def at(h, l, x, c):
    return {"dp": 2 * h + l, "tensor": 2 * x + c}


def flip(value, by):
    return (value + by) % 2


def shift(h, by, planes):
    return (h + by) % planes


class Mail:
    def __init__(self, send, recv):
        self.send_sems, self.recv_sems = send, recv
        self.sent = 0
        self.todo = []

    def copy(self, src, dst, target, slot):
        return pltpu.make_async_remote_copy(
            src_ref=src, dst_ref=dst, send_sem=self.send_sems.at[self.sent], recv_sem=self.recv_sems.at[slot],
            device_id=target, device_id_type=pl.DeviceIdType.MESH,
        )

    def post(self, src, dst, target, slot, keep=None, local=None):
        copy = self.copy(src, dst, target, slot)
        self.sent += 1
        if keep is None:
            copy.start()
        else:
            pl.when(jnp.logical_not(keep))(copy.start)
            if local is not None:
                pl.when(keep)(local)
        self.todo.append((copy, keep))

    def drain(self):
        for copy, keep in self.todo:
            if keep is None:
                copy.wait_send()
            else:
                pl.when(jnp.logical_not(keep))(copy.wait_send)
        self.todo = []

    def take(self, dst, target, slot, keep=None):
        copy = pltpu.make_async_remote_copy(
            src_ref=dst, dst_ref=dst, send_sem=self.send_sems.at[0], recv_sem=self.recv_sems.at[slot],
            device_id=target, device_id_type=pl.DeviceIdType.MESH,
        )
        if keep is None:
            copy.wait_recv()
        else:
            pl.when(jnp.logical_not(keep))(copy.wait_recv)


def greet(peers):
    barrier = pltpu.get_barrier_semaphore()
    for peer in peers:
        pl.semaphore_signal(barrier, inc=1, device_id=peer, device_id_type=pl.DeviceIdType.MESH)
    pl.semaphore_wait(barrier, len(peers))


def plane_peers(me):
    return [
        at(me.h, flip(me.l, fl), flip(me.x, fx), flip(me.c, fc))
        for fl in (0, 1) for fx in (0, 1) for fc in (0, 1) if fl + fx + fc
    ]


def column_peers(me):
    return [
        at(shift(me.h, dh, me.planes), flip(me.l, fl), me.x, flip(me.c, fc))
        for dh in range(1, me.planes) for fl in (0, 1) for fc in (0, 1)
    ]


def line_peers(me):
    return [
        at(shift(me.h, dh, me.planes), flip(me.l, fl), me.x, me.c)
        for dh in range(me.planes) for fl in (0, 1) if dh + fl
    ]


def sibling(me):
    return at(me.h, me.l, me.x, flip(me.c, 1))


def call(body, name, number, data_count, arrays, outs, sends, recvs, limit=None):
    def kernel(*refs):
        count = len(arrays)
        ins, rest = refs[:count], refs[count:]
        body(Seat(data_count), Mail(rest[-2], rest[-1]), ins, rest[:len(outs)])

    return pl.pallas_call(
        kernel,
        out_shape=tuple(jax.ShapeDtypeStruct(*o) for o in outs),
        in_specs=[pl.BlockSpec(memory_space=pltpu.VMEM)] * len(arrays),
        out_specs=(pl.BlockSpec(memory_space=pltpu.VMEM),) * len(outs),
        scratch_shapes=[pltpu.SemaphoreType.DMA((sends,)), pltpu.SemaphoreType.DMA((recvs,))],
        compiler_params=pltpu.CompilerParams(collective_id=number, has_side_effects=True),
        name=name,
    )(*arrays)


def begin_body(me, mail, ins, outs):
    vec, win, rows_in, cot_in = ins
    vec_all, weights, chip_in, chip_cot = outs
    planes = me.planes
    greet(plane_peers(me) + column_peers(me))
    vec_slot = lambda i: i
    z_slot = lambda i: 8 + i
    w_slot = lambda i: 8 + planes + i
    r_slot = 8 + 3 * planes
    for fl in (0, 1):
        for fx in (0, 1):
            for fc in (0, 1):
                if fl + fx + fc:
                    mail.post(vec, vec_all.at[me.h, me.spot], at(me.h, flip(me.l, fl), flip(me.x, fx), flip(me.c, fc)), vec_slot(me.spot))
    vec_all[me.h, me.spot] = vec[...]
    mine = me.l == me.c

    def keep_weights():
        weights[me.d] = win[...]

    for dh in range(planes):
        for fc in (0, 1):
            local = dh + fc == 0
            mail.post(win, weights.at[me.d], at(shift(me.h, dh, planes), me.c, me.x, flip(me.c, fc)), w_slot(me.d),
                      mine if local else None, keep_weights if local else None)
    mail.post(rows_in, chip_in.at[me.c], sibling(me), r_slot)
    mail.post(cot_in, chip_cot.at[me.c], sibling(me), r_slot + 1)
    chip_in[me.c] = rows_in[...]
    chip_cot[me.c] = cot_in[...]
    for fl in (0, 1):
        for fx in (0, 1):
            for fc in (0, 1):
                if fl + fx + fc:
                    l, x, c = flip(me.l, fl), flip(me.x, fx), flip(me.c, fc)
                    spot = 4 * l + 2 * x + c
                    mail.take(vec_all.at[me.h, spot], at(me.h, l, x, c), vec_slot(spot))
    for dh in range(1, planes):
        mail.post(vec_all.at[me.h], vec_all.at[me.h], at(shift(me.h, dh, planes), me.l, me.x, me.c), z_slot(me.h))
    for dh in range(1, planes):
        h = shift(me.h, dh, planes)
        mail.take(vec_all.at[h], at(h, me.l, me.x, me.c), z_slot(h))
    for dh in range(planes):
        for fl in (0, 1):
            h, l = shift(me.h, dh, planes), flip(me.l, fl)
            mail.take(weights.at[2 * h + l], at(h, l, me.x, me.l), w_slot(2 * h + l), mine if dh + fl == 0 else None)
    other = flip(me.c, 1)
    mail.take(chip_in.at[other], sibling(me), r_slot)
    mail.take(chip_cot.at[other], sibling(me), r_slot + 1)
    mail.drain()


def rows_body(me, mail, ins, outs):
    (block,), (rows,) = ins, outs
    greet(plane_peers(me))
    mine = me.l == me.c

    def keep():
        rows[me.t] = block[...]

    for fl in (0, 1):
        for fx in (0, 1):
            local = fl + fx == 0
            mail.post(block, rows.at[me.t], at(me.h, flip(me.l, fl), flip(me.x, fx), me.l), me.t,
                      mine if local else None, keep if local else None)
    for fx in (0, 1):
        for fc in (0, 1):
            x, c = flip(me.x, fx), flip(me.c, fc)
            mail.take(rows.at[2 * x + c], at(me.h, me.c, x, c), 2 * x + c, mine if fx + fc == 0 else None)
    mail.drain()


def run_seat(me, run):
    return at(run // 2, me.l, me.x, run % 2)


def edges(me, mail, pairs, left_slot, right_slot):
    last = 2 * me.planes - 1
    has_left, has_right = me.run > 0, me.run < last
    left, right = run_seat(me, jnp.maximum(me.run - 1, 0)), run_seat(me, jnp.minimum(me.run + 1, last))
    barrier = pltpu.get_barrier_semaphore()
    for has, peer in ((has_left, left), (has_right, right)):
        @pl.when(has)
        def _(peer=peer):
            pl.semaphore_signal(barrier, inc=1, device_id=peer, device_id_type=pl.DeviceIdType.MESH)
    pl.semaphore_wait(barrier, jnp.where(has_left, 1, 0) + jnp.where(has_right, 1, 0))
    (to_left, land_left), (to_right, land_right) = pairs
    mail.post(to_left, land_left, left, 1, jnp.logical_not(has_left))
    mail.post(to_right, land_right, right, 0, jnp.logical_not(has_right))
    for has, slot in ((has_left, left_slot), (has_right, right_slot)):
        @pl.when(jnp.logical_not(has))
        def _(slot=slot):
            slot[...] = jnp.zeros(slot.shape, slot.dtype)
    return has_left, has_right, left, right


def halo_body(me, mail, ins, outs):
    (own,), (ext,) = ins, outs
    pairs = ((own, ext.at[2]), (own, ext.at[0]))
    has_left, has_right, left, right = edges(me, mail, pairs, ext.at[0], ext.at[2])
    ext[1] = own[...]
    mail.take(ext.at[0], left, 0, jnp.logical_not(has_left))
    mail.take(ext.at[2], right, 1, jnp.logical_not(has_right))
    mail.drain()


def rims_body(me, mail, ins, outs):
    (rim,), (got,) = ins, outs
    pairs = ((rim.at[0], got.at[1]), (rim.at[1], got.at[0]))
    has_left, has_right, left, right = edges(me, mail, pairs, got.at[0], got.at[1])
    mail.take(got.at[0], left, 0, jnp.logical_not(has_left))
    mail.take(got.at[1], right, 1, jnp.logical_not(has_right))
    mail.drain()


def swap_body(outward, me, mail, ins, outs):
    (parts,), (got,) = ins, outs
    mine = me.l == me.c
    barrier = pltpu.get_barrier_semaphore()
    cross = at(me.h, me.c, me.x, me.l)
    pl.semaphore_signal(barrier, inc=1, device_id=at(me.h, me.c, flip(me.x, 1), me.l), device_id_type=pl.DeviceIdType.MESH)

    @pl.when(jnp.logical_not(mine))
    def _():
        pl.semaphore_signal(barrier, inc=1, device_id=cross, device_id_type=pl.DeviceIdType.MESH)

    pl.semaphore_wait(barrier, jnp.where(mine, 1, 2))
    for fx in (0, 1):
        x = flip(me.x, fx)
        src = parts.at[x] if outward else parts.at[fx]
        dst = got.at[fx] if outward else got.at[me.x]
        slot = fx

        def keep(fx=fx, x=x):
            if outward:
                got[fx] = parts[x]
            else:
                got[me.x] = parts[fx]

        mail.post(src, dst, at(me.h, me.c, x, me.l), slot, mine if fx == 0 else None, keep if fx == 0 else None)
    for fx in (0, 1):
        x = flip(me.x, fx)
        mail.take(got.at[fx] if outward else got.at[x], at(me.h, me.c, x, me.l), fx, mine if fx == 0 else None)
    mail.drain()


def pair_body(me, mail, ins, outs):
    greet([sibling(me)])
    for i, (src, dst) in enumerate(zip(ins, outs)):
        mail.post(src, dst, sibling(me), i)
    for i, dst in enumerate(outs):
        mail.take(dst, sibling(me), i)
    mail.drain()


def return_body(me, mail, ins, outs):
    rows, grads = ins
    got_rows, got_grads = outs
    planes = me.planes
    greet(plane_peers(me) + column_peers(me))
    mine = me.l == me.c
    corner = 2 * me.l + me.x

    def keep_rows():
        got_rows[corner] = rows[me.t]

    def keep_grads():
        got_grads[me.run] = grads[me.d]

    for fx in (0, 1):
        for fc in (0, 1):
            x, c = flip(me.x, fx), flip(me.c, fc)
            local = fx + fc == 0
            mail.post(rows.at[2 * x + c], got_rows.at[corner], at(me.h, me.c, x, c), corner,
                      mine if local else None, keep_rows if local else None)
    for dh in range(planes):
        for fl in (0, 1):
            h, l = shift(me.h, dh, planes), flip(me.l, fl)
            local = dh + fl == 0
            mail.post(grads.at[2 * h + l], got_grads.at[me.run], at(h, l, me.x, me.l), 4 + me.run,
                      mine if local else None, keep_grads if local else None)
    for fl in (0, 1):
        for fx in (0, 1):
            l, x = flip(me.l, fl), flip(me.x, fx)
            mail.take(got_rows.at[2 * l + x], at(me.h, l, x, me.l), 2 * l + x, mine if fl + fx == 0 else None)
    for dh in range(planes):
        for fc in (0, 1):
            h, c = shift(me.h, dh, planes), flip(me.c, fc)
            mail.take(got_grads.at[2 * h + c], at(h, me.c, me.x, c), 4 + 2 * h + c, mine if dh + fc == 0 else None)
    mail.drain()


def owner_plane(kind, planes):
    return kind * planes // 4


def collect_body(me, mail, ins, outs):
    states, vec = ins
    block, got_vec = outs
    planes = me.planes
    block[...] = jnp.zeros(block.shape, block.dtype)
    greet(line_peers(me))
    count = 2 * planes
    for dh in range(planes):
        for fl in (0, 1):
            h, l = shift(me.h, dh, planes), flip(me.l, fl)
            if dh + fl:
                mail.post(vec.at[2 * h + l], got_vec.at[me.d], at(h, l, me.x, me.c), count + me.d)
    got_vec[me.d] = vec[me.d]
    for kind in range(4):
        home = owner_plane(kind, planes)
        for fl in (0, 1):
            l = flip(me.l, fl)

            def keep(kind=kind):
                block[me.d] = states[kind, me.l]

            mail.post(states.at[kind, l], block.at[me.d], at(home, l, me.x, me.c), me.d,
                      (me.h == home) if fl == 0 else None, keep if fl == 0 else None)
    idle = (me.h * 4) % planes != 0
    for dh in range(planes):
        for fl in (0, 1):
            h, l = shift(me.h, dh, planes), flip(me.l, fl)
            if dh + fl:
                mail.take(block.at[2 * h + l], at(h, l, me.x, me.c), 2 * h + l, idle)
                mail.take(got_vec.at[2 * h + l], at(h, l, me.x, me.c), count + 2 * h + l)
    mail.drain()


def spots(me):
    for fl in (0, 1):
        for fx in (0, 1):
            for fc in (0, 1):
                if fl + fx + fc:
                    l, x, c = flip(me.l, fl), flip(me.x, fx), flip(me.c, fc)
                    yield 4 * l + 2 * x + c, at(me.h, l, x, c)


def scatter_body(me, mail, ins, outs):
    terms, vec = ins
    got, got_vec = outs
    greet(plane_peers(me))
    for spot, seat in spots(me):
        mail.post(terms.at[spot], got.at[me.spot], seat, me.spot)
    for fx in (0, 1):
        for fc in (0, 1):
            if fx + fc:
                x, c = flip(me.x, fx), flip(me.c, fc)
                mail.post(vec.at[2 * x + c], got_vec.at[me.t], at(me.h, me.l, x, c), 8 + me.t)
    got[me.spot] = terms[me.spot]
    got_vec[me.t] = vec[me.t]
    for spot, seat in spots(me):
        mail.take(got.at[spot], seat, spot)
    for fx in (0, 1):
        for fc in (0, 1):
            if fx + fc:
                x, c = flip(me.x, fx), flip(me.c, fc)
                mail.take(got_vec.at[2 * x + c], at(me.h, me.l, x, c), 8 + 2 * x + c)
    mail.drain()


def share_body(me, mail, ins, outs):
    (block,), (got,) = ins, outs
    greet(plane_peers(me))
    for spot, seat in spots(me):
        mail.post(block, got.at[me.spot], seat, me.spot)
    got[me.spot] = block[...]
    for spot, seat in spots(me):
        mail.take(got.at[spot], seat, spot)
    mail.drain()


def deliver_body(me, mail, ins, outs):
    (blocks,), (got,) = ins, outs
    planes = me.planes
    greet(line_peers(me))
    kind = me.h * 4 // planes
    idle = (me.h * 4) % planes != 0
    for dh in range(planes):
        for fl in (0, 1):
            h, l = shift(me.h, dh, planes), flip(me.l, fl)
            if dh + fl:
                mail.post(blocks.at[2 * h + l], got.at[kind, me.l], at(h, l, me.x, me.c), 2 * kind + me.l, idle)

    @pl.when(jnp.logical_not(idle))
    def _():
        got[kind, me.l] = blocks[me.d]

    for other in range(4):
        home = owner_plane(other, planes)
        for fl in (0, 1):
            l = flip(me.l, fl)
            mail.take(got.at[other, l], at(home, l, me.x, me.c), 2 * other + l, (me.h == home) if fl == 0 else None)
    mail.drain()


def normalize(values_in):
    center = values_in - jnp.mean(values_in, axis=-1, keepdims=True)
    inverse = lax.rsqrt(jnp.mean(center * center, axis=-1, keepdims=True) + norm_epsilon)
    return (center * inverse, inverse)


def norm_back(grad_rows, unit, inverse, gain):
    scaled = grad_rows * gain
    return inverse * (
        scaled
        - jnp.mean(scaled, axis=-1, keepdims=True)
        - unit * jnp.mean(scaled * unit, axis=-1, keepdims=True)
    )


def gelu_value(pre):
    return pre * 0.5 * (1.0 + lax.erf(pre * root_half))


def gelu_slope(pre):
    return 0.5 * (1.0 + lax.erf(pre * root_half)) + pre * jnp.exp(-0.5 * pre * pre) * gauss_factor


def narrow(value):
    return value.astype(jnp.bfloat16)


def wide(value):
    return value.astype(jnp.float32)


def mul(left, right):
    return jnp.dot(left, right, preferred_element_type=jnp.float32)


def orthogonalize(gram, block):
    norm = jnp.sqrt(jnp.trace(gram)) + frobenius_epsilon
    gram = narrow(gram / (norm * norm))
    state = narrow(wide(block) / norm)
    for sweep in range(NS_STEPS):
        poly = narrow(quintic_two * wide(gram) + quintic_three * mul(gram, gram))
        state = narrow(quintic_one * wide(state) + mul(poly, state))
        if sweep < NS_STEPS - 1:
            half = narrow(quintic_one * wide(gram) + mul(poly, gram))
            gram = narrow(quintic_one * wide(half) + mul(half, poly))
    return state


def head_slots(values, heads, offset):
    grid = values.reshape(values.shape[0], heads, HDIM)
    return jnp.pad(grid, ((0, 0), (0, 0), (offset, LANES - HDIM - offset))).reshape(values.shape[0], heads * LANES)


def halves(matrix, room):
    rows, cols = matrix.shape
    grid = narrow(matrix).reshape(rows, 2, cols // 2).transpose(1, 0, 2)
    return jnp.pad(grid, ((0, 0), (0, 0), (0, room - cols // 2)))


def whole(pair, cols):
    return pair[:, :, : cols // 2].transpose(1, 0, 2).reshape(pair.shape[1], cols)


def local(
    inputs,
    cotangent,
    clip_lengths,
    inward_weight,
    outward_weight,
    expand_weight,
    shrink_weight,
    gains,
    shifts,
    biases,
    expand_bias,
    inward_moment,
    outward_moment,
    expand_moment,
    shrink_moment,
    gains_moment,
    shifts_moment,
    biases_moment,
    expand_bias_moment,
):
    data_count = lax.axis_size("dp")
    tensor_count = lax.axis_size("tensor")
    devices = data_count * tensor_count
    planes = data_count // 2
    assert tensor_count == 4 and planes % 4 == 0
    data_at = lax.axis_index("dp")
    tensor_at = lax.axis_index("tensor")
    plane_at, level = data_at // 2, data_at % 2
    column, core = tensor_at // 2, tensor_at % 2
    rows, width = inputs.shape
    run = rows * tensor_count
    assert run >= MAXCLIP
    chip = 2 * rows
    run_at = 2 * plane_at + core
    shard = inward_weight.shape[0]
    head_cols = inward_weight.shape[2]
    heads = head_cols // HDIM
    slots = heads * LANES
    hidden = expand_weight.shape[1]
    hidden_width = hidden * tensor_count
    group = 2 * column + level
    twin = (tensor_at + 2) % tensor_count
    piece = width // devices
    hidden_piece = hidden_width // devices
    vec_size = 8 * piece + hidden_piece
    scale = 1.0 / math.sqrt(HDIM)
    to_twin = [(i, (i + 2) % tensor_count) for i in range(tensor_count)]

    def talk(body, name, number, arrays, outs, sends, recvs):
        return call(body, name, number, data_count, arrays, outs, sends, recvs)

    def gather_weights(packed):
        mine = lax.all_gather(packed, "dp", axis=0, tiled=True)
        return mine, lax.ppermute(mine, "tensor", to_twin)

    packed_vec = jnp.concatenate([gains.reshape(-1), shifts.reshape(-1), biases.reshape(-1), expand_bias])
    packed_vec = jnp.pad(packed_vec, (0, 1024 - vec_size)).reshape(8, LANES)
    section = narrow(inward_weight).reshape(shard, 3, heads, HDIM)
    blank = jnp.zeros((shard, heads, HDIM), jnp.bfloat16)
    inward_packed = jnp.concatenate(
        [
            jnp.concatenate([section[:, 0], blank], axis=2).reshape(shard, slots),
            jnp.concatenate([section[:, 1], section[:, 2]], axis=2).reshape(shard, slots),
        ],
        axis=1,
    )
    vec_all, inward_full, chip_in, chip_cot = talk(
        begin_body,
        "begin",
        1,
        (packed_vec, inward_packed, inputs, cotangent),
        (
            ((planes, 8, 8, LANES), jnp.float32),
            ((data_count, shard, 2 * slots), jnp.bfloat16),
            ((2, rows, width), jnp.float32),
            ((2, rows, width), jnp.float32),
        ),
        7 + 2 * planes + 2 + planes - 1,
        8 + 3 * planes + 2,
    )
    table = vec_all.reshape(devices, 1024)

    def spread(first, count, size):
        return table[:, first : first + count * size].reshape(devices, count, size).transpose(1, 0, 2).reshape(count, -1)

    full_gains = spread(0, 2, piece)
    full_shifts = spread(2 * piece, 2, piece)
    full_biases = spread(4 * piece, 4, piece)
    full_hidden = spread(8 * piece, 1, hidden_piece)[0]
    chip_in = chip_in.reshape(chip, width)
    chip_cot = chip_cot.reshape(chip, width)
    inward_full = inward_full.reshape(width, 2 * slots)
    query_w, pair_w = inward_full[:, :slots], inward_full[:, slots:]

    unit_one, inverse_one = normalize(inputs)
    normed_one = narrow(unit_one * full_gains[0] + full_shifts[0])
    (rows_run,) = talk(rows_body, "rows", 2, (normed_one,), (((4, rows, width), jnp.bfloat16),), 4, 4)
    rows_run = rows_run.reshape(run, width)
    up_shard = jnp.concatenate([narrow(expand_weight), narrow(outward_weight).T], axis=1)
    up_mine, up_twin = gather_weights(up_shard)
    down_mine, down_twin = gather_weights(narrow(shrink_weight).T)

    def group_slice(row):
        return lax.dynamic_slice_in_dim(row, group * head_cols, head_cols)[None]

    query_bias = head_slots(group_slice(full_biases[0]), heads, 0)
    pair_bias = head_slots(group_slice(full_biases[1]), heads, HDIM)
    query = narrow(mul(rows_run, query_w) + query_bias) * jnp.bfloat16(scale)
    pairs = narrow(mul(rows_run, pair_w) + pair_bias)
    (extended,) = talk(halo_body, "halo", 3, (pairs,), (((3, run, slots), jnp.bfloat16),), 2, 2)
    extended = extended.reshape(3 * run, slots)
    base = (run_at * run).astype(jnp.int32).reshape(1)
    attended, log_totals = attend_forward(clip_lengths, base, query, extended, heads, 768, 512)
    (attended_chip,) = talk(
        functools.partial(swap_body, True), "swap_out", 4, (attended.reshape(2, chip, head_cols),),
        (((2, chip, head_cols), jnp.bfloat16),), 2, 2,
    )

    out_mine, out_twin = up_mine[:, hidden:], up_twin[:, hidden:]
    expand_mine, expand_twin = up_mine[:, :hidden], up_twin[:, :hidden]
    out_part = narrow(over_last(attended_chip[0], out_mine) + over_last(attended_chip[1], out_twin))
    (out_other,) = talk(pair_body, "pair_mid", 5, (out_part,), (((chip, width), jnp.bfloat16),), 1, 1)
    mid = chip_in + (wide(out_part) + wide(out_other)) + full_biases[2]
    unit_two, inverse_two = normalize(mid)
    rows_two = narrow(unit_two * full_gains[1] + full_shifts[1])
    grad_b = narrow(chip_cot)
    hidden_mine = lax.dynamic_slice_in_dim(full_hidden, tensor_at * hidden, hidden)
    hidden_twin = lax.dynamic_slice_in_dim(full_hidden, twin * hidden, hidden)

    def feed(expand_w, shrink_w, bias):
        pre = mul(rows_two, expand_w) + bias
        act = narrow(gelu_value(pre))
        pre_grad = mul(grad_b, shrink_w) * gelu_slope(pre)
        return act, narrow(pre_grad), jnp.sum(pre_grad, axis=0)

    act_mine, pre_mine, hidden_sum_mine = feed(expand_mine, down_mine, hidden_mine)
    act_twin, pre_twin, hidden_sum_twin = feed(expand_twin, down_twin, hidden_twin)
    feed_part = narrow(over_last(act_mine, down_mine) + over_last(act_twin, down_twin))
    back_part = narrow(over_last(pre_mine, expand_mine) + over_last(pre_twin, expand_twin))
    feed_away = lax.dynamic_slice_in_dim(feed_part, (1 - core) * rows, rows, 0)
    feed_home = lax.dynamic_slice_in_dim(feed_part, core * rows, rows, 0)
    feed_other, back_other = talk(
        pair_body, "pair_feed", 6, (feed_away, back_part),
        (((rows, width), jnp.bfloat16), ((chip, width), jnp.bfloat16)), 2, 2,
    )
    output = (
        lax.dynamic_slice_in_dim(mid, core * rows, rows, 0) + (wide(feed_home) + wide(feed_other)) + full_biases[3]
    )
    normed_two_grad = wide(back_part) + wide(back_other)
    mid_grad = chip_cot + norm_back(normed_two_grad, unit_two, inverse_two, full_gains[1])
    mid_grad_b = narrow(mid_grad)

    def reduce_over(mine, away):
        got = lax.ppermute(narrow(away), "tensor", to_twin)
        return wide(lax.psum_scatter(narrow(mine + wide(got)), "dp", scatter_dimension=0, tiled=True))

    shrink_shard = reduce_over(over_first(grad_b, act_mine), over_first(grad_b, act_twin))
    expand_shard = reduce_over(over_first(rows_two, pre_mine), over_first(rows_two, pre_twin))
    outward_shard = reduce_over(
        over_first(mid_grad_b, attended_chip[0]), over_first(mid_grad_b, attended_chip[1])
    )

    attended_grad = jnp.stack([narrow(mul(mid_grad_b, out_mine)), narrow(mul(mid_grad_b, out_twin))])
    (attended_grad,) = talk(
        functools.partial(swap_body, False), "swap_back", 7, (attended_grad,),
        (((2, chip, head_cols), jnp.bfloat16),), 2, 2,
    )
    query_grad, pair_own, rims, _ = attend_backward(
        clip_lengths, base, query, extended, attended, attended_grad.reshape(run, head_cols), log_totals, heads, 256, 512
    )
    (arrived,) = talk(rims_body, "rims", 8, (rims,), (((2, run, slots), jnp.bfloat16),), 2, 2)
    pair_grad = pair_own + wide(arrived[0]) + wide(arrived[1])
    pair_grad_b = narrow(pair_grad)
    row_terms = narrow(over_last(query_grad, query_w) + over_last(pair_grad_b, pair_w))
    inward_terms = jnp.concatenate(
        [narrow(over_first(rows_run, query_grad)), narrow(over_first(rows_run, pair_grad_b))], axis=1
    )
    got_rows, got_inward = talk(
        return_body, "give_back", 9,
        (row_terms.reshape(4, rows, width), inward_terms.reshape(data_count, shard, 2 * slots)),
        (((4, rows, width), jnp.bfloat16), ((data_count, shard, 2 * slots), jnp.bfloat16)),
        4 + 2 * planes, 4 + 2 * planes,
    )
    normed_one_grad = jnp.sum(wide(got_rows), axis=0)
    inward_sum = jnp.sum(wide(got_inward), axis=0)
    mid_grad_own = lax.dynamic_slice_in_dim(mid_grad, core * rows, rows, 0)
    input_grad = mid_grad_own + norm_back(normed_one_grad, unit_one, inverse_one, full_gains[0])
    grid = inward_sum.reshape(shard, 2, heads, LANES)
    inward_grad = jnp.stack(
        [
            grid[:, 0, :, :HDIM].reshape(shard, head_cols),
            grid[:, 1, :, :HDIM].reshape(shard, head_cols),
            grid[:, 1, :, HDIM:].reshape(shard, head_cols),
        ],
        axis=1,
    )

    def placed(row, first, size):
        return lax.dynamic_update_slice_in_dim(jnp.zeros((size,), jnp.float32), row, first, 0)

    query_sum = jnp.sum(wide(query_grad), axis=0).reshape(heads, LANES)[:, :HDIM].reshape(-1)
    value_sum = jnp.sum(pair_grad, axis=0).reshape(heads, LANES)[:, HDIM:].reshape(-1)
    vec_terms = jnp.stack(
        [
            jnp.sum(normed_one_grad * unit_one, axis=0),
            0.5 * jnp.sum(normed_two_grad * unit_two, axis=0),
            jnp.sum(normed_one_grad, axis=0),
            0.5 * jnp.sum(normed_two_grad, axis=0),
            placed(query_sum, group * head_cols, width),
            placed(value_sum, group * head_cols, width),
            0.5 * jnp.sum(mid_grad, axis=0),
            jnp.sum(cotangent, axis=0),
        ]
    )
    hidden_terms = placed(hidden_sum_mine, tensor_at * hidden, hidden_width) + placed(
        hidden_sum_twin, twin * hidden, hidden_width
    )
    vec_terms = jnp.concatenate(
        [vec_terms.reshape(8, devices, piece).transpose(1, 0, 2).reshape(devices, 8 * piece),
         hidden_terms.reshape(devices, hidden_piece)],
        axis=1,
    )
    vec_terms = jnp.pad(vec_terms, ((0, 0), (0, 1024 - vec_size))).reshape(data_count, 4, 8, LANES)

    outward_turned = outward_shard.T
    shrink_turned = shrink_shard.T
    inward_state = momentum_decay * inward_moment + inward_grad
    outward_state = momentum_decay * outward_moment + outward_turned
    expand_state = momentum_decay * expand_moment + expand_shard
    shrink_state = momentum_decay * shrink_moment + shrink_turned
    room = hidden // 2
    states = jnp.stack(
        [
            halves(inward_state.reshape(shard, 3 * head_cols), room),
            halves(outward_state.T, room),
            halves(expand_state, room),
            halves(shrink_state.T, room),
        ]
    )
    block, got_vec = talk(
        collect_body, "collect", 10, (states, vec_terms),
        (((data_count, shard, room), jnp.bfloat16), ((data_count, 4, 8, LANES), jnp.float32)),
        2 * planes - 1 + 8, 4 * planes,
    )
    block = block.reshape(width, room)
    gram_terms = narrow(over_last(block, block)).reshape(8, width // 8, width)
    got_gram, got_vec = talk(
        scatter_body, "gram_sum", 11, (gram_terms, jnp.sum(got_vec, axis=0)),
        (((8, width // 8, width), jnp.bfloat16), ((4, 8, LANES), jnp.float32)), 10, 12,
    )
    (gram,) = talk(
        share_body, "gram_share", 12, (narrow(jnp.sum(wide(got_gram), axis=0)),),
        (((8, width // 8, width), jnp.bfloat16),), 7, 8,
    )
    ortho = orthogonalize(wide(gram.reshape(width, width)), block)
    (mine,) = talk(
        deliver_body, "deliver", 13, (ortho.reshape(data_count, shard, room),),
        (((4, 2, shard, room), jnp.bfloat16),), 2 * planes - 1, 8,
    )
    ortho_in = wide(whole(mine[0], 3 * head_cols)).reshape(inward_weight.shape)
    ortho_out = wide(whole(mine[1], head_cols)).T
    ortho_up = wide(whole(mine[2], hidden))
    ortho_down = wide(whole(mine[3], hidden)).T
    inward_new = inward_weight - learn_rate * 0.2 * math.sqrt(3 * width) * ortho_in
    outward_new = outward_weight - learn_rate * 0.2 * math.sqrt(width) * ortho_out
    expand_new = expand_weight - learn_rate * 0.2 * math.sqrt(max(width, hidden_width)) * ortho_up
    shrink_new = shrink_weight - learn_rate * 0.2 * math.sqrt(max(width, hidden_width)) * ortho_down

    vec = jnp.sum(got_vec, axis=0).reshape(-1)
    gains_grad = vec[: 2 * piece].reshape(2, piece)
    shifts_grad = vec[2 * piece : 4 * piece].reshape(2, piece)
    biases_grad = vec[4 * piece : 8 * piece].reshape(4, piece)
    expand_bias_grad = vec[8 * piece : vec_size]
    gains_state = momentum_decay * gains_moment + gains_grad
    shifts_state = momentum_decay * shifts_moment + shifts_grad
    biases_state = momentum_decay * biases_moment + biases_grad
    expand_bias_state = momentum_decay * expand_bias_moment + expand_bias_grad
    gains_new = gains - vector_rate * gains_state
    shifts_new = shifts - vector_rate * shifts_state
    biases_new = biases - vector_rate * biases_state
    expand_bias_new = expand_bias - vector_rate * expand_bias_state
    return (
        output,
        input_grad,
        inward_grad,
        outward_turned,
        expand_shard,
        shrink_turned,
        gains_grad,
        shifts_grad,
        biases_grad,
        expand_bias_grad,
        inward_new,
        outward_new,
        expand_new,
        shrink_new,
        gains_new,
        shifts_new,
        biases_new,
        expand_bias_new,
        inward_state,
        outward_state,
        expand_state,
        shrink_state,
        gains_state,
        shifts_state,
        biases_state,
        expand_bias_state,
    )


def solution(mesh):
    in_specs = (
        P(("dp", "tensor"), None),
        P(("dp", "tensor"), None),
        P(),
        P("dp", None, "tensor"),
        P("tensor", "dp"),
        P("dp", "tensor"),
        P("tensor", "dp"),
        P(None, ("dp", "tensor")),
        P(None, ("dp", "tensor")),
        P(None, ("dp", "tensor")),
        P(("dp", "tensor")),
        P("dp", None, "tensor"),
        P("tensor", "dp"),
        P("dp", "tensor"),
        P("tensor", "dp"),
        P(None, ("dp", "tensor")),
        P(None, ("dp", "tensor")),
        P(None, ("dp", "tensor")),
        P(("dp", "tensor")),
    )
    out_specs = (
        P(("dp", "tensor"), None),
        P(("dp", "tensor"), None),
        P("dp", None, "tensor"),
        P("tensor", "dp"),
        P("dp", "tensor"),
        P("tensor", "dp"),
        P(None, ("dp", "tensor")),
        P(None, ("dp", "tensor")),
        P(None, ("dp", "tensor")),
        P(("dp", "tensor")),
        P("dp", None, "tensor"),
        P("tensor", "dp"),
        P("dp", "tensor"),
        P("tensor", "dp"),
        P(None, ("dp", "tensor")),
        P(None, ("dp", "tensor")),
        P(None, ("dp", "tensor")),
        P(("dp", "tensor")),
        P("dp", None, "tensor"),
        P("tensor", "dp"),
        P("dp", "tensor"),
        P("tensor", "dp"),
        P(None, ("dp", "tensor")),
        P(None, ("dp", "tensor")),
        P(None, ("dp", "tensor")),
        P(("dp", "tensor")),
    )
    return jax.shard_map(local, mesh=mesh, in_specs=in_specs, out_specs=out_specs, check_vma=False)
```
